32 devices in a mesh: fsdp: 16 (over z, y, core), tp: 2 (over x).
Axes of the slice: x: 2, y: 2, z: 4, core: 2. Of those that a mesh axis runs over, the one named last changes fastest.
Arguments:
- hidden: bfloat16 [32, 5120], P(None, 'fsdp'), may hold values from -20 to 20
- query_weight: bfloat16 [5120, 5120], P(None, ('tp', 'fsdp')), may hold values from -0.078125 to 0.078125
- key_weight: bfloat16 [5120, 1024], P(None, ('tp', 'fsdp')), may hold values from -0.078125 to 0.078125
- value_weight: bfloat16 [5120, 1024], P(None, ('tp', 'fsdp')), may hold values from -0.078125 to 0.078125
- output_weight: bfloat16 [5120, 5120], P(('tp', 'fsdp')), may hold values from -0.078125 to 0.078125
- gate_weight: bfloat16 [5120, 27648], P(None, ('tp', 'fsdp')), may hold values from -0.078125 to 0.078125
- up_weight: bfloat16 [5120, 27648], P(None, ('tp', 'fsdp')), may hold values from -0.078125 to 0.078125
- down_weight: bfloat16 [27648, 5120], P(('tp', 'fsdp')), may hold values from -0.0390625 to 0.0390625
- history: float32 [7, 1024], replicated, may hold values from 0.0001 to 1, as said below
- slot: int32 [1], replicated, may hold values from 0 to 1023
- lengths: int32 [32], P('fsdp'), may hold values from 512 to 4096, as said below
- key_cache: bfloat16 [32, 4096, 1024], P('fsdp', None, 'tp'), may hold values from -1000 to 1000
- value_cache: bfloat16 [32, 4096, 1024], P('fsdp', None, 'tp'), may hold values from -6 to 6
Outputs:
- attention_out: bfloat16 [32, 5120], P('fsdp', 'tp')
- query_rollout: bfloat16 [5120, 5120], P('fsdp', 'tp')
- key_rollout: bfloat16 [5120, 1024], P('fsdp', 'tp')
- value_rollout: bfloat16 [5120, 1024], P('fsdp', 'tp')
- output_rollout: bfloat16 [5120, 5120], P('tp', 'fsdp')
- gate_rollout: bfloat16 [5120, 27648], P('fsdp', 'tp')
- up_rollout: bfloat16 [5120, 27648], P('fsdp', 'tp')
- down_rollout: bfloat16 [27648, 5120], P('tp', 'fsdp')
- new_history: float32 [7, 1024], replicated
The draws below stay inside these ranges and needn't reach their ends.
Inputs may be any that keep to these rules, and one draw needn't show every extreme that they name: `history`: strictly positive. `lengths`: some sequence has all 4096 slots valid.
All inputs are finite; a program needn't handle non-finite values.
Results may differ from the reference program's by a relative error of at most 0.012.
The reference program's roundings to bfloat16 on the way (of `probs`) count: a program that leaves them out, or rounds other values in their place, can miss the bound.
Values may be sent and summed in bfloat16 or wider, within the bound.
A program may use at most 192 MiB of HBM per device.

```python
import jax
import jax.numpy as jnp
from jax import lax

D = 5120
F = 27648
HEADS = 40
KV_HEADS = 8
HEAD_DIM = 128
HIST = 1024
CACHE = 4096
SEQS = 32


def draw_hidden(key, part):
    values = jnp.clip(jax.random.normal(jax.random.fold_in(key, 11), (SEQS, D), jnp.float32), -6.0, 6.0)
    return values.astype(jnp.bfloat16)


def draw_history(key, part):
    fans = jnp.array([D, D, D, D, D, D, F], jnp.float32)
    low, high = (3.0, 12.0)
    levels = jnp.exp(jax.random.uniform(jax.random.fold_in(key, 21), (7,), jnp.float32, jnp.log(low), jnp.log(high)))
    spread = jnp.exp(jax.random.uniform(jax.random.fold_in(key, 22), (7, HIST), jnp.float32, jnp.log(0.02), 0.0))
    return (fans ** (-0.5) * levels)[:, None] * spread


def draw_lengths(key, part):
    counts = jax.random.randint(jax.random.fold_in(key, 31), (SEQS,), CACHE // 8, CACHE + 1)
    chosen = jax.random.randint(jax.random.fold_in(key, 32), (), 0, SEQS)
    return jnp.where(jnp.arange(SEQS) == chosen, CACHE, counts).astype(jnp.int32)


def draw_key_cache(key, part):
    values = jnp.clip(jax.random.normal(jax.random.fold_in(key, 41), (SEQS, CACHE, KV_HEADS * HEAD_DIM), jnp.float32), -6.0, 6.0)
    return values.astype(jnp.bfloat16)


def block_scale(own_key, shape, cuts, low, top_value):
    level, own = 1.0, jax.random.fold_in(own_key, 6)
    for dim, shards_of in cuts:
        heights = jnp.exp(jax.random.uniform(jax.random.fold_in(own, dim), (shards_of,), jnp.float32, low / len(cuts), top_value / len(cuts)))
        level = level * jnp.repeat(heights, shape[dim] // shards_of).reshape([-1 if axis == dim else 1 for axis in range(len(shape))])
    return level


def scatter_about(rng, extent, width, reach, cuts=(), kind=jnp.bfloat16):
    loudness = block_scale(rng, extent, cuts, -0.22, 0.18) if cuts else 1.0
    values = jax.random.normal(rng, extent, jnp.float32) * width * loudness
    return jnp.minimum(jnp.maximum(values, -reach), reach).astype(kind)


def setup_inputs(seed: int = 0) -> dict:
    streams_of = jax.random.split(jax.random.key(seed), 14)
    hidden = draw_hidden(jax.random.fold_in(streams_of[13], 71), 0)
    query_weight = scatter_about(streams_of[1], (D, D), D ** -0.5, 0.078125, ((1, 32),))
    key_weight = scatter_about(streams_of[2], (D, KV_HEADS * HEAD_DIM), D ** -0.5, 0.078125, ((1, 32),))
    value_weight = scatter_about(streams_of[3], (D, KV_HEADS * HEAD_DIM), D ** -0.5, 0.078125, ((1, 32),))
    output_weight = scatter_about(streams_of[4], (D, D), D ** -0.5, 0.078125, ((0, 32),))
    gate_weight = scatter_about(streams_of[5], (D, F), D ** -0.5, 0.078125, ((1, 32),))
    up_weight = scatter_about(streams_of[6], (D, F), D ** -0.5, 0.078125, ((1, 32),))
    down_weight = scatter_about(streams_of[7], (F, D), F ** -0.5, 0.0390625, ((0, 32),))
    history = draw_history(jax.random.fold_in(streams_of[13], 71), 0)
    slot = jax.random.randint(streams_of[9], (1,), 0, HIST).astype(jnp.int32)
    lengths = draw_lengths(jax.random.fold_in(streams_of[13], 71), 0)
    key_cache = draw_key_cache(jax.random.fold_in(streams_of[13], 71), 0)
    value_cache = scatter_about(streams_of[12], (SEQS, CACHE, KV_HEADS * HEAD_DIM), 1.0, 6.0, ((0, 16), (2, 2)))
    return dict(hidden=hidden, query_weight=query_weight, key_weight=key_weight, value_weight=value_weight, output_weight=output_weight, gate_weight=gate_weight, up_weight=up_weight, down_weight=down_weight, history=history, slot=slot, lengths=lengths, key_cache=key_cache, value_cache=value_cache)


target_peak = 4.0
norm_eps = 1e-06
rope_theta = 1000000.0

def largest(tensor):
    return jnp.max(jnp.abs(tensor.astype(jnp.float32)))

def scaling(peaks, history, slot):
    marked = lax.broadcasted_iota(jnp.int32, history.shape, 1) == slot[0]
    kept = lax.optimization_barrier(jnp.max(jnp.where(marked, jnp.zeros_like(history), history), axis=1))
    return (target_peak / jnp.maximum(peaks, kept), jnp.where(marked, peaks[:, None], history))

def quantize(tensor, factor):
    return (tensor.astype(jnp.float32) * factor).astype(jnp.bfloat16)

def rotate(vectors, positions):
    half_dim = vectors.shape[-1] // 2
    ladder = jnp.arange(half_dim, dtype=jnp.float32)
    spread = rope_theta ** (-2.0 * ladder / vectors.shape[-1])
    angle = positions.astype(jnp.float32)[:, None] * spread[None, :]
    cosine = jnp.cos(angle)[:, None, :]
    sine = jnp.sin(angle)[:, None, :]
    first = vectors[..., :half_dim]
    second = vectors[..., half_dim:]
    return jnp.concatenate([first * cosine - second * sine, second * cosine + first * sine], axis=-1)

def one_sequence(items):
    query, key_new, value_new, cached_keys, cached_values, length = items
    kv_count = query.shape[0]
    head_dim = query.shape[2]
    cache_len = cached_keys.shape[0]
    keys = cached_keys.reshape(cache_len, kv_count, head_dim).astype(jnp.float32)
    values = cached_values.reshape(cache_len, kv_count, head_dim).astype(jnp.float32)
    scale = head_dim ** (-0.5)
    widened = query.astype(jnp.float32)
    scores = jnp.einsum('kgd,jkd->kgj', widened, keys) * scale
    own = lax.optimization_barrier(jnp.sum(widened * key_new.astype(jnp.float32)[:, None, :], axis=-1)) * scale
    valid = (lax.broadcasted_iota(jnp.int32, (cache_len,), 0) < length)[None, None, :]
    top = jnp.maximum(lax.optimization_barrier(jnp.max(jnp.where(valid, scores, -1e+30), axis=-1)), own)
    weights = jnp.where(valid, jnp.exp(scores - top[..., None]), 0.0)
    own_weight = jnp.exp(own - top)
    total = lax.optimization_barrier(jnp.sum(weights, axis=-1)) + own_weight
    probs = (weights / total[..., None]).astype(jnp.bfloat16)
    own_prob = (own_weight / total).astype(jnp.bfloat16)
    mixed = jnp.einsum('kgj,jkd->kgd', probs.astype(jnp.float32), values)
    mixed = mixed + own_prob.astype(jnp.float32)[..., None] * value_new.astype(jnp.float32)[:, None, :]
    return mixed.astype(jnp.bfloat16).reshape(-1)

def reference(hidden, query_weight, key_weight, value_weight, output_weight, gate_weight, up_weight, down_weight, history, slot, lengths, key_cache, value_cache):
    trainer = [query_weight, key_weight, value_weight, output_weight, gate_weight, up_weight, down_weight]
    peaks = jnp.stack([largest(tensor) for tensor in trainer])
    factors, new_history = scaling(peaks, history, slot)
    rollout = [quantize(trainer[number], factors[number]) for number in range(7)]
    widened = hidden.astype(jnp.float32)
    inv_rms = lax.rsqrt(lax.optimization_barrier(jnp.mean(widened * widened, axis=1)) + norm_eps)[:, None]
    query = jnp.dot(hidden, rollout[0], preferred_element_type=jnp.float32) * inv_rms / factors[0]
    key_new = jnp.dot(hidden, rollout[1], preferred_element_type=jnp.float32) * inv_rms / factors[1]
    value_new = jnp.dot(hidden, rollout[2], preferred_element_type=jnp.float32) * inv_rms / factors[2]
    count_seq = hidden.shape[0]
    query = rotate(query.reshape(count_seq, HEADS, HEAD_DIM), lengths).astype(jnp.bfloat16)
    query = query.reshape(count_seq, KV_HEADS, HEADS // KV_HEADS, HEAD_DIM)
    key_new = rotate(key_new.reshape(count_seq, KV_HEADS, HEAD_DIM), lengths).astype(jnp.bfloat16)
    value_new = value_new.reshape(count_seq, KV_HEADS, HEAD_DIM).astype(jnp.bfloat16)
    attention_out = lax.map(one_sequence, (query, key_new, value_new, key_cache, value_cache, lengths))
    return (attention_out, rollout[0], rollout[1], rollout[2], rollout[3], rollout[4], rollout[5], rollout[6], new_history)
```

```python
import jax
import jax.numpy as jnp
from jax import lax
from jax.sharding import PartitionSpec as P

D = 5120
HEADS = 40
KV_HEADS = 8
HEAD_DIM = 128


target_peak = 4.0
norm_eps = 1e-06
rope_theta = 1000000.0


def largest(tensor):
    return jnp.max(jnp.abs(tensor.astype(jnp.float32)))


def scaling(peaks, history, slot):
    marked = lax.broadcasted_iota(jnp.int32, history.shape, 1) == slot[0]
    kept = jnp.max(jnp.where(marked, jnp.zeros_like(history), history), axis=1)
    return (target_peak / jnp.maximum(peaks, kept), jnp.where(marked, peaks[:, None], history))


def quantize(tensor, factor):
    return (tensor.astype(jnp.float32) * factor).astype(jnp.bfloat16)


def rotate(vectors, positions):
    half_dim = vectors.shape[-1] // 2
    ladder = jnp.arange(half_dim, dtype=jnp.float32)
    spread = rope_theta ** (-2.0 * ladder / vectors.shape[-1])
    angle = positions.astype(jnp.float32)[:, None] * spread[None, :]
    cosine = jnp.cos(angle)[:, None, :]
    sine = jnp.sin(angle)[:, None, :]
    first = vectors[..., :half_dim]
    second = vectors[..., half_dim:]
    return jnp.concatenate(
        [first * cosine - second * sine, second * cosine + first * sine], axis=-1
    )


def after(tensor, *earlier):
    return lax.optimization_barrier((tensor,) + earlier)[0]


def exchange_columns(part, *earlier):
    count = lax.axis_size("fsdp")
    rows, width = part.shape
    blocks = lax.optimization_barrier(part.reshape(count, rows // count, width))
    return lax.all_to_all(
        after(blocks, *earlier), "fsdp", split_axis=0, concat_axis=0, tiled=True
    )


def beside(blocks):
    count, rows, width = blocks.shape
    return blocks.transpose(1, 0, 2).reshape(rows, count * width)


def exchange_rows(part, *earlier):
    count = lax.axis_size("fsdp")
    rows, width = part.shape
    blocks = lax.optimization_barrier(
        part.reshape(rows, count, width // count).transpose(1, 0, 2)
    )
    return lax.all_to_all(
        after(blocks, *earlier), "fsdp", split_axis=0, concat_axis=0, tiled=True
    )


def below(blocks):
    count, rows, width = blocks.shape
    return blocks.reshape(count * rows, width)


def attend(query, key_new, value_new, key_cache, value_cache, lengths):
    count_seq = query.shape[0]
    kv_count = query.shape[1]
    head_dim = query.shape[3]
    cache_len = key_cache.shape[1]
    keys = key_cache.reshape(count_seq, cache_len, kv_count, head_dim)
    values = value_cache.reshape(count_seq, cache_len, kv_count, head_dim)
    scale = head_dim ** (-0.5)
    scores = jnp.einsum("bkgd,bjkd->bkgj", query, keys, preferred_element_type=jnp.float32) * scale
    own = (
        jnp.sum(query.astype(jnp.float32) * key_new.astype(jnp.float32)[:, :, None, :], axis=-1)
        * scale
    )
    valid = (lax.broadcasted_iota(jnp.int32, (count_seq, cache_len), 1) < lengths[:, None])[
        :, None, None, :
    ]
    top = jnp.maximum(jnp.max(jnp.where(valid, scores, -1e30), axis=-1), own)
    weights = jnp.where(valid, jnp.exp(scores - top[..., None]), 0.0)
    own_weight = jnp.exp(own - top)
    total = jnp.sum(weights, axis=-1) + own_weight
    probs = (weights / total[..., None]).astype(jnp.bfloat16)
    own_prob = (own_weight / total).astype(jnp.bfloat16)
    mixed = jnp.einsum("bkgj,bjkd->bkgd", probs, values, preferred_element_type=jnp.float32)
    mixed = (
        mixed
        + own_prob.astype(jnp.float32)[..., None] * value_new.astype(jnp.float32)[:, :, None, :]
    )
    return mixed.astype(jnp.bfloat16).reshape(count_seq, -1)


def per_device(
    hidden,
    query_weight,
    key_weight,
    value_weight,
    output_weight,
    gate_weight,
    up_weight,
    down_weight,
    history,
    slot,
    lengths,
    key_cache,
    value_cache,
):
    trainer = (
        query_weight,
        key_weight,
        value_weight,
        output_weight,
        gate_weight,
        up_weight,
        down_weight,
    )
    wide_q, wide_k = query_weight.shape[1], key_weight.shape[1]
    packed = exchange_columns(jnp.concatenate([query_weight, key_weight, value_weight], axis=1))
    local = after(jnp.stack([largest(tensor) for tensor in trainer]), packed)
    peaks = lax.pmax(local, ("fsdp", "tp"))
    factors, new_history = scaling(peaks, history, slot)
    gate_blocks = exchange_columns(gate_weight, peaks)
    query_rollout = quantize(beside(packed[:, :, :wide_q]), factors[0])
    key_rollout = quantize(beside(packed[:, :, wide_q : wide_q + wide_k]), factors[1])
    value_rollout = quantize(beside(packed[:, :, wide_q + wide_k :]), factors[2])
    widened = hidden.astype(jnp.float32)
    squares = jnp.sum(widened * widened, axis=1)
    joined = jnp.concatenate([query_rollout, key_rollout, value_rollout], axis=1)
    partial_value = jnp.dot(hidden, joined, preferred_element_type=jnp.float32)
    summed = lax.psum_scatter(
        jnp.concatenate([partial_value, squares[:, None]], axis=1),
        "fsdp",
        scatter_dimension=0,
        tiled=True,
    )
    up_blocks = exchange_columns(up_weight, gate_blocks, summed)
    gate_rollout = quantize(beside(gate_blocks), factors[4])
    total_sq = summed[:, -1]
    summed = summed[:, :-1]
    inv_rms = lax.rsqrt(total_sq / D + norm_eps)[:, None]
    width_q = query_rollout.shape[1]
    width_k = key_rollout.shape[1]
    query = summed[:, :width_q] * inv_rms / factors[0]
    key_new = summed[:, width_q : width_q + width_k] * inv_rms / factors[1]
    value_new = summed[:, width_q + width_k :] * inv_rms / factors[2]
    count_seq = summed.shape[0]
    query = rotate(query.reshape(count_seq, -1, HEAD_DIM), lengths).astype(jnp.bfloat16)
    query = query.reshape(count_seq, -1, HEADS // KV_HEADS, HEAD_DIM)
    key_new = rotate(key_new.reshape(count_seq, -1, HEAD_DIM), lengths).astype(jnp.bfloat16)
    value_new = value_new.reshape(count_seq, -1, HEAD_DIM).astype(jnp.bfloat16)
    attention_out = attend(query, key_new, value_new, key_cache, value_cache, lengths)
    down_arrived = exchange_rows(down_weight, up_blocks, gate_rollout, attention_out)
    up_rollout = quantize(beside(up_blocks), factors[5])
    output_arrived = exchange_rows(output_weight, down_arrived, up_rollout)
    down_rollout = quantize(below(down_arrived), factors[6])
    output_rollout = quantize(below(output_arrived), factors[3])
    return (
        attention_out,
        query_rollout,
        key_rollout,
        value_rollout,
        output_rollout,
        gate_rollout,
        up_rollout,
        down_rollout,
        new_history,
    )


def solution(mesh):
    return jax.shard_map(
        per_device,
        mesh=mesh,
        in_specs=(
            P(None, "fsdp"),
            P(None, ("tp", "fsdp")),
            P(None, ("tp", "fsdp")),
            P(None, ("tp", "fsdp")),
            P(("tp", "fsdp"), None),
            P(None, ("tp", "fsdp")),
            P(None, ("tp", "fsdp")),
            P(("tp", "fsdp"), None),
            P(),
            P(),
            P("fsdp"),
            P("fsdp", None, "tp"),
            P("fsdp", None, "tp"),
        ),
        out_specs=(
            P("fsdp", "tp"),
            P("fsdp", "tp"),
            P("fsdp", "tp"),
            P("fsdp", "tp"),
            P("tp", "fsdp"),
            P("fsdp", "tp"),
            P("fsdp", "tp"),
            P("tp", "fsdp"),
            P(),
        ),
        check_vma=False,
    )
```
